32 devices in a mesh: fsdp: 8 (over z, y), seq: 4 (over x, core).
Axes of the slice: x: 2, y: 2, z: 4, core: 2. Of those that a mesh axis runs over, the one named last changes fastest.
Arguments:
- tokens: bfloat16 [8, 1024, 1152], P('fsdp', 'seq'), may hold values from -6 to 6
- condition: float32 [8, 1152], P('fsdp'), may hold values from -6 to 6
- w_ada: bfloat16 [1152, 6912], P('fsdp'), may hold values from -0.1875 to 0.1875
- b_ada: bfloat16 [6912], P('fsdp'), may hold values from -3 to 3
- w_qkv: bfloat16 [1152, 3456], P('fsdp'), may hold values from -0.1875 to 0.1875
- b_qv: bfloat16 [2, 1152], P(None, 'fsdp'), may hold values from -3 to 3
- w_out: bfloat16 [1152, 1152], P('fsdp'), may hold values from -0.75 to 0.75
- b_out: bfloat16 [1152], P('fsdp'), may hold values from -3 to 3
- w_up: bfloat16 [1152, 4608], P('fsdp'), may hold values from -0.1875 to 0.1875
- b_up: bfloat16 [4608], P('fsdp'), may hold values from -3 to 3
- w_down: bfloat16 [4608, 1152], P('fsdp'), may hold values from -0.09375 to 0.09375
- b_down: bfloat16 [1152], P('fsdp'), may hold values from -3 to 3
- grad_output: bfloat16 [8, 1024, 1152], P('fsdp', 'seq'), may hold values from -6 to 6
Outputs:
- output: bfloat16 [8, 1024, 1152], P('fsdp', 'seq')
- grad_tokens: bfloat16 [8, 1024, 1152], P('fsdp', 'seq')
- grad_condition: float32 [8, 1152], P('fsdp')
- grad_w_ada: float32 [1152, 6912], P('fsdp')
- grad_b_ada: float32 [6912], P('fsdp')
- grad_w_qkv: float32 [1152, 3456], P('fsdp')
- grad_b_qv: float32 [2, 1152], P(None, 'fsdp')
- grad_w_out: float32 [1152, 1152], P('fsdp')
- grad_b_out: float32 [1152], P('fsdp')
- grad_w_up: float32 [1152, 4608], P('fsdp')
- grad_b_up: float32 [4608], P('fsdp')
- grad_w_down: float32 [4608, 1152], P('fsdp')
- grad_b_down: float32 [1152], P('fsdp')
The draws below stay inside these ranges and needn't reach their ends.
All inputs are finite; a program needn't handle non-finite values.
Results may differ from the reference program's by a relative error of at most 0.018.
Values may be sent and summed in bfloat16 or wider, within the bound.
A program may use at most 320 MiB of HBM per device.

```python
import jax
import jax.numpy as jnp
from jax import lax

D = 1152
HEADS = 16
HD = 72
FF = 4608
SEQ_LEN = 1024
ATT = 1152
LATENTS = 8
MODS = 6912
N_SEQ = 4


def levels(key, extent, split, smallest, largest):
    gain = 1.0
    for axis_at, blocks in split:
        steps = jax.random.uniform(jax.random.fold_in(jax.random.fold_in(key, 6), axis_at), (blocks,), jnp.float32, smallest / len(split), largest / len(split))
        gain = gain * jnp.repeat(jnp.exp(steps), extent[axis_at] // blocks).reshape((-1,) + (1,) * (len(extent) - 1 - axis_at))
    return gain


def gaussian(own_key, extent, scale, most, split=(), dtype=jnp.bfloat16):
    gain = levels(own_key, extent, split, -0.22, 0.18) if split else 1.0
    array = jax.random.normal(own_key, extent, jnp.float32) * scale * gain
    return jnp.minimum(jnp.maximum(array, -most), most).astype(dtype)


def setup_inputs(seed: int = 0) -> dict:
    streams_of = jax.random.split(jax.random.key(seed), 14)
    tokens = gaussian(streams_of[0], (LATENTS, SEQ_LEN, D), 1.0, 6.0, ((0, 8), (1, 4)))
    condition = gaussian(streams_of[1], (LATENTS, D), 1.0, 6.0, ((0, 8),), jnp.float32)
    w_ada = gaussian(streams_of[2], (D, MODS), D ** -0.5, 0.1875, ((0, 8),))
    b_ada = gaussian(streams_of[3], (MODS,), 0.5, 3.0, ((0, 8),))
    w_qkv = gaussian(streams_of[4], (D, 3 * ATT), D ** -0.5, 0.1875, ((0, 8),))
    b_qv = gaussian(streams_of[5], (2, ATT), 0.5, 3.0, ((1, 8),))
    w_out = gaussian(streams_of[6], (ATT, D), (ATT * 64 // SEQ_LEN) ** -0.5, 0.75, ((0, 8),))
    b_out = gaussian(streams_of[7], (D,), 0.5, 3.0, ((0, 8),))
    w_up = gaussian(streams_of[8], (D, FF), D ** -0.5, 0.1875, ((0, 8),))
    b_up = gaussian(streams_of[9], (FF,), 0.5, 3.0, ((0, 8),))
    w_down = gaussian(streams_of[10], (FF, D), FF ** -0.5, 0.09375, ((0, 8),))
    b_down = gaussian(streams_of[11], (D,), 0.5, 3.0, ((0, 8),))
    grad_output = gaussian(streams_of[12], (LATENTS, SEQ_LEN, D), 1.0, 6.0, ((0, 8), (1, 4)))
    return {"tokens": tokens, "condition": condition, "w_ada": w_ada, "b_ada": b_ada, "w_qkv": w_qkv, "b_qv": b_qv, "w_out": w_out, "b_out": b_out, "w_up": w_up, "b_up": b_up, "w_down": w_down, "b_down": b_down, "grad_output": grad_output}


EPSILON = 1e-06
GELU_C = 0.7978845608028654
HIGH = lax.Precision.HIGHEST

def layer_norm(values):
    mean_val = lax.optimization_barrier(jnp.mean(values, axis=-1, keepdims=True))
    centred = values - mean_val
    inv_std = lax.rsqrt(lax.optimization_barrier(jnp.mean(centred * centred, axis=-1, keepdims=True)) + EPSILON)
    return (centred * inv_std, inv_std)

def norm_back(grad_norm, normed, inv_std):
    first = lax.optimization_barrier(jnp.mean(grad_norm, axis=-1, keepdims=True))
    second = lax.optimization_barrier(jnp.mean(grad_norm * normed, axis=-1, keepdims=True))
    return inv_std * (grad_norm - first - normed * second)

def gelu_tanh(values):
    inner = GELU_C * (values + 0.044715 * values * values * values)
    return 0.5 * values * (1.0 + jnp.tanh(inner))

def gelu_slope(values):
    inner = GELU_C * (values + 0.044715 * values * values * values)
    tanh_val = jnp.tanh(inner)
    return 0.5 * (1.0 + tanh_val) + 0.5 * values * (1.0 - tanh_val * tanh_val) * GELU_C * (1.0 + 3.0 * 0.044715 * values * values)

def head_scores(query, key):
    factor = HD ** (-0.5)
    return jnp.einsum('qhd,khd->hqk', query.astype(jnp.float32), key.astype(jnp.float32), precision=HIGH) * factor

def attend_all(query, key, value):
    scores = head_scores(query, key)
    highest = lax.optimization_barrier(jnp.max(scores, axis=-1, keepdims=True))
    log_total = highest + jnp.log(lax.optimization_barrier(jnp.sum(jnp.exp(scores - highest), axis=-1, keepdims=True)))
    probs = jnp.exp(scores - log_total).astype(jnp.bfloat16)
    mixed = jnp.einsum('hqk,khd->qhd', probs.astype(jnp.float32), value.astype(jnp.float32), precision=HIGH)
    return (mixed.astype(jnp.bfloat16), log_total)

def attend_back(query, key, value, mixed, log_total, grad_mix):
    factor = HD ** (-0.5)
    probs = jnp.exp(head_scores(query, key) - log_total)
    delta = lax.optimization_barrier(jnp.sum(grad_mix.astype(jnp.float32) * mixed.astype(jnp.float32), axis=-1))
    grad_probs = jnp.einsum('qhd,khd->hqk', grad_mix.astype(jnp.float32), value.astype(jnp.float32), precision=HIGH)
    grad_scores = (probs * (grad_probs - jnp.transpose(delta)[:, :, None]) * factor).astype(jnp.bfloat16).astype(jnp.float32)
    grad_query = jnp.einsum('hqk,khd->qhd', grad_scores, key.astype(jnp.float32), precision=HIGH)
    grad_key = jnp.einsum('hqk,qhd->khd', grad_scores, query.astype(jnp.float32), precision=HIGH)
    probs_low = probs.astype(jnp.bfloat16).astype(jnp.float32)
    grad_value = jnp.einsum('hqk,qhd->khd', probs_low, grad_mix.astype(jnp.float32), precision=HIGH)
    return (grad_query.astype(jnp.bfloat16), grad_key.astype(jnp.bfloat16), grad_value.astype(jnp.bfloat16))

def block_sums(values):
    return lax.optimization_barrier(jnp.sum(values.reshape(N_SEQ, SEQ_LEN // N_SEQ, D), axis=1))

def dot_tn(left, right):
    return lax.dot_general(left, right, (((0,), (0,)), ((), ())), preferred_element_type=jnp.float32)

def dot_nt(left, right):
    return lax.dot_general(left, right, (((1,), (1,)), ((), ())), preferred_element_type=jnp.float32)

def latent_pass(source_low, grad_low, mods, weights):
    w_qkv, b_qv, w_out, b_out, w_up, b_up, w_down, b_down = weights
    shift_attn, scale_attn, gate_attn = (mods[0], mods[1], mods[2])
    shift_ff, scale_ff, gate_ff = (mods[3], mods[4], mods[5])
    source = source_low.astype(jnp.float32)
    normed1, inv1 = layer_norm(source)
    hidden1 = (normed1 * (1.0 + scale_attn) + shift_attn).astype(jnp.bfloat16)
    qkv = jnp.dot(hidden1, w_qkv, preferred_element_type=jnp.float32)
    query = (qkv[:, :ATT] + b_qv[0].astype(jnp.float32)).astype(jnp.bfloat16)
    key = qkv[:, ATT:2 * ATT].astype(jnp.bfloat16)
    value = (qkv[:, 2 * ATT:] + b_qv[1].astype(jnp.float32)).astype(jnp.bfloat16)
    shape_heads = (SEQ_LEN, HEADS, HD)
    query_h = query.reshape(shape_heads)
    key_h = key.reshape(shape_heads)
    value_h = value.reshape(shape_heads)
    mixed_h, log_total = attend_all(query_h, key_h, value_h)
    attn_mix = mixed_h.reshape(SEQ_LEN, ATT)
    attn_out = jnp.dot(attn_mix, w_out, preferred_element_type=jnp.float32) + b_out.astype(jnp.float32)
    resid1 = source + gate_attn * attn_out
    normed2, inv2 = layer_norm(resid1)
    hidden2 = (normed2 * (1.0 + scale_ff) + shift_ff).astype(jnp.bfloat16)
    pre_act = jnp.dot(hidden2, w_up, preferred_element_type=jnp.float32) + b_up.astype(jnp.float32)
    activated = gelu_tanh(pre_act).astype(jnp.bfloat16)
    ff_out = jnp.dot(activated, w_down, preferred_element_type=jnp.float32) + b_down.astype(jnp.float32)
    output = (resid1 + gate_ff * ff_out).astype(jnp.bfloat16)
    grad_y = grad_low.astype(jnp.float32)
    grad_ff = grad_y * gate_ff
    grad_ff_low = grad_ff.astype(jnp.bfloat16)
    grad_w_down = dot_tn(activated, grad_ff_low)
    grad_b_down = lax.optimization_barrier(jnp.sum(grad_ff, axis=0))
    grad_pre = dot_nt(grad_ff_low, w_down) * gelu_slope(pre_act)
    grad_pre_low = grad_pre.astype(jnp.bfloat16)
    grad_w_up = dot_tn(hidden2, grad_pre_low)
    grad_b_up = lax.optimization_barrier(jnp.sum(grad_pre, axis=0))
    grad_h2 = dot_nt(grad_pre_low, w_up)
    grad_resid1 = grad_y + norm_back(grad_h2 * (1.0 + scale_ff), normed2, inv2)
    grad_attn = grad_resid1 * gate_attn
    grad_attn_low = grad_attn.astype(jnp.bfloat16)
    grad_w_out = dot_tn(attn_mix, grad_attn_low)
    grad_b_out = lax.optimization_barrier(jnp.sum(grad_attn, axis=0))
    grad_mix = dot_nt(grad_attn_low, w_out).astype(jnp.bfloat16)
    grad_q, grad_k, grad_v = attend_back(query_h, key_h, value_h, mixed_h, log_total, grad_mix.reshape(shape_heads))
    grad_qkv = jnp.concatenate([grad_q.reshape(SEQ_LEN, ATT), grad_k.reshape(SEQ_LEN, ATT), grad_v.reshape(SEQ_LEN, ATT)], axis=1)
    grad_w_qkv = dot_tn(hidden1, grad_qkv)
    grad_b_qv = jnp.stack([lax.optimization_barrier(jnp.sum(grad_qkv[:, :ATT].astype(jnp.float32), axis=0)), lax.optimization_barrier(jnp.sum(grad_qkv[:, 2 * ATT:].astype(jnp.float32), axis=0))])
    grad_h1 = dot_nt(grad_qkv, w_qkv)
    grad_x = (grad_resid1 + norm_back(grad_h1 * (1.0 + scale_attn), normed1, inv1)).astype(jnp.bfloat16)
    mods_part = jnp.stack([block_sums(grad_h1), block_sums(grad_h1 * normed1), block_sums(grad_resid1 * attn_out), block_sums(grad_h2), block_sums(grad_h2 * normed2), block_sums(grad_y * ff_out)], axis=1)
    grads = (grad_w_qkv, grad_b_qv, grad_w_out, grad_b_out, grad_w_up, grad_b_up, grad_w_down, grad_b_down)
    return (output, grad_x, mods_part.reshape(N_SEQ, 6 * D), grads)

def reference(tokens, condition, w_ada, b_ada, w_qkv, b_qv, w_out, b_out, w_up, b_up, w_down, b_down, grad_output):
    cond_sig = jax.nn.sigmoid(condition)
    cond_act = (condition * cond_sig).astype(jnp.bfloat16)
    mods = jnp.dot(cond_act, w_ada, preferred_element_type=jnp.float32) + b_ada.astype(jnp.float32)
    mods = mods.reshape(LATENTS, 6, D)
    weights = (w_qkv, b_qv, w_out, b_out, w_up, b_up, w_down, b_down)
    zeros = tuple((jnp.zeros(weight.shape, jnp.float32) for weight in weights))

    def scan_step(carry, items):
        source_low, grad_low, latent_mods = items
        output, grad_x, mods_part, grads = latent_pass(source_low, grad_low, latent_mods, weights)
        return (tuple((held + added for held, added in zip(carry, grads))), (output, grad_x, mods_part))
    totals, (outputs, grad_xs, parts) = lax.scan(scan_step, zeros, (tokens, grad_output, mods))
    parts_low = parts.astype(jnp.bfloat16).astype(jnp.float32)
    grad_b_ada = lax.optimization_barrier(jnp.sum(parts_low, axis=(0, 1)))
    mods_sum = lax.optimization_barrier(jnp.sum(parts_low, axis=1))
    grad_w_ada = jnp.dot(jnp.transpose(cond_act.astype(jnp.float32)), mods_sum, precision=HIGH)
    grad_cond_act = jnp.dot(mods_sum, jnp.transpose(w_ada.astype(jnp.float32)), precision=HIGH)
    grad_condition = grad_cond_act * cond_sig * (1.0 + condition * (1.0 - cond_sig))
    return (outputs, grad_xs, grad_condition, grad_w_ada, grad_b_ada, totals[0], totals[1], totals[2], totals[3], totals[4], totals[5], totals[6], totals[7])
```

```python
import functools

import jax
import jax.numpy as jnp
from jax import lax
from jax.experimental import pallas as pl
from jax.experimental.pallas import tpu as pltpu
from jax.sharding import PartitionSpec as P

HD = 72
EPSILON = 1e-06
GELU_C = 0.7978845608028654
SCALE = HD**-0.5
BF = jnp.bfloat16
F32 = jnp.float32
VMEM_LIMIT = 60 * 1024 * 1024


def dot(left, right):
    return jnp.dot(left, right, preferred_element_type=F32)


def dot_nt(left, right):
    return lax.dot_general(left, right, (((1,), (1,)), ((), ())), preferred_element_type=F32)


def dot_tn(left, right):
    return lax.dot_general(left, right, (((0,), (0,)), ((), ())), preferred_element_type=F32)


def rows_of(block, size):
    return pl.ds(pl.multiple_of(block * size, size), size)


def layer_norm(values):
    mean_val = jnp.mean(values, axis=-1, keepdims=True)
    centred = values - mean_val
    inv_std = lax.rsqrt(jnp.mean(centred * centred, axis=-1, keepdims=True) + EPSILON)
    return (centred * inv_std, inv_std)


def norm_back(grad_norm, normed, inv_std):
    first = jnp.mean(grad_norm, axis=-1, keepdims=True)
    second = jnp.mean(grad_norm * normed, axis=-1, keepdims=True)
    return inv_std * (grad_norm - first - normed * second)


def attn_kernel(heads, block, h_ref, w_ref, b_ref, wo_ref, part_ref, qkv_ref, mix_ref, lse_ref):
    total = h_ref.shape[0]
    steps = total // block

    def project(step, carry):
        at = rows_of(step, block)
        qkv = (dot(h_ref[at, :], w_ref[...]) + b_ref[...]).astype(BF)
        for j in range(3 * heads):
            qkv_ref[j, at, :] = qkv[:, j * HD : (j + 1) * HD]
        return carry

    lax.fori_loop(0, steps, project, 0)

    def attend(step, carry):
        at = rows_of(step, block)
        mixed, lses = [], []
        for h in range(heads):
            scores = dot_nt(qkv_ref[h, at, :], qkv_ref[heads + h, :, :])
            highest = jnp.max(scores, axis=-1, keepdims=True)
            weights = jnp.exp((scores - highest) * SCALE)
            total_w = jnp.sum(weights, axis=-1, keepdims=True)
            probs = (weights * (1.0 / total_w)).astype(BF)
            mixed.append(dot(probs, qkv_ref[2 * heads + h, :, :]).astype(BF))
            lses.append(highest * SCALE + jnp.log(total_w))
        mix = jnp.concatenate(mixed, axis=1)
        mix_ref[at, :] = mix
        lse_ref[at, :] = jnp.concatenate(lses, axis=1)
        part_ref[at, :] = dot(mix, wo_ref[...]).astype(BF)
        return carry

    lax.fori_loop(0, steps, attend, 0)


def attn_forward(hidden, w_qkv, bias, w_out):
    total, width = hidden.shape
    inner = w_out.shape[0]
    heads = inner // HD
    vmem = pl.BlockSpec(memory_space=pltpu.VMEM)
    return pl.pallas_call(
        functools.partial(attn_kernel, heads, 256),
        out_shape=(
            jax.ShapeDtypeStruct((total, width), BF),
            jax.ShapeDtypeStruct((3 * heads, total, HD), BF),
            jax.ShapeDtypeStruct((total, inner), BF),
            jax.ShapeDtypeStruct((total, heads), F32),
        ),
        in_specs=[vmem] * 4,
        out_specs=(vmem,) * 4,
        compiler_params=pltpu.CompilerParams(vmem_limit_bytes=VMEM_LIMIT),
        cost_estimate=pl.CostEstimate(
            flops=2 * total * width * inner * 4 + 4 * total * total * heads * 128,
            bytes_accessed=2 * (2 * total * width + 4 * width * inner + 5 * total * inner),
            transcendentals=heads * total * total,
        ),
        name="attn_forward",
    )(hidden, w_qkv, bias, w_out)


def attn_back_kernel(
    heads, block, ga_ref, h_ref, w_ref, wo_ref, qkv_ref, mix_ref, lse_ref,
    gh_ref, gw_ref, gwo_ref, gb_ref, gqkv_ref, gk_acc, gv_acc,
):
    total, width = h_ref.shape
    inner = wo_ref.shape[0]
    steps = total // block
    gk_acc[...] = jnp.zeros_like(gk_acc)
    gv_acc[...] = jnp.zeros_like(gv_acc)

    def attend(step, carry):
        at = rows_of(step, block)
        grad_mix = dot_nt(ga_ref[at, :], wo_ref[...]).astype(BF)
        mix = mix_ref[at, :]
        lse = lse_ref[at, :]
        grads = []
        for h in range(heads):
            here = slice(h * HD, (h + 1) * HD)
            gm = grad_mix[:, here]
            query = qkv_ref[h, at, :]
            key = qkv_ref[heads + h, :, :]
            scores = dot_nt(query, key)
            probs = jnp.exp(scores * SCALE - lse[:, h : h + 1])
            delta = jnp.sum(gm.astype(F32) * mix[:, here].astype(F32), axis=-1, keepdims=True)
            grad_p = dot_nt(gm, qkv_ref[2 * heads + h, :, :])
            grad_s = (probs * (grad_p - delta) * SCALE).astype(BF)
            grads.append(dot(grad_s, key).astype(BF))
            gk_acc[h] += dot_tn(grad_s, query)
            gv_acc[h] += dot_tn(probs.astype(BF), gm)
        gqkv_ref[at, :inner] = jnp.concatenate(grads, axis=1)
        return carry

    lax.fori_loop(0, steps, attend, 0)
    gqkv_ref[:, inner : 2 * inner] = jnp.concatenate(
        [gk_acc[h].astype(BF) for h in range(heads)], axis=1
    )
    gqkv_ref[:, 2 * inner :] = jnp.concatenate(
        [gv_acc[h].astype(BF) for h in range(heads)], axis=1
    )

    def weight(step, carry):
        at = rows_of(step, 384)
        gw_ref[at, :] = dot_tn(h_ref[:, at], gqkv_ref[...]).astype(BF)
        return carry

    lax.fori_loop(0, width // 384, weight, 0)
    gwo_ref[...] = dot_tn(mix_ref[...], ga_ref[...]).astype(BF)

    def hidden(step, sums):
        at = rows_of(step, block)
        part = gqkv_ref[at, :]
        gh_ref[at, :] = dot_nt(part, w_ref[...]).astype(BF)
        return sums + jnp.sum(part.astype(F32), axis=0, keepdims=True)

    gb_ref[...] = lax.fori_loop(0, steps, hidden, jnp.zeros((1, 3 * inner), F32))


def attn_backward(grad_attn, hidden, w_qkv, w_out, qkv, mix, lse):
    total, width = hidden.shape
    inner = w_out.shape[0]
    heads = inner // HD
    vmem = pl.BlockSpec(memory_space=pltpu.VMEM)
    return pl.pallas_call(
        functools.partial(attn_back_kernel, heads, 256),
        out_shape=(
            jax.ShapeDtypeStruct((total, width), BF),
            jax.ShapeDtypeStruct((width, 3 * inner), BF),
            jax.ShapeDtypeStruct((inner, width), BF),
            jax.ShapeDtypeStruct((1, 3 * inner), F32),
        ),
        in_specs=[vmem] * 7,
        out_specs=(vmem,) * 4,
        scratch_shapes=[
            pltpu.VMEM((total, 3 * inner), BF),
            pltpu.VMEM((heads, total, HD), F32),
            pltpu.VMEM((heads, total, HD), F32),
        ],
        compiler_params=pltpu.CompilerParams(vmem_limit_bytes=VMEM_LIMIT),
        cost_estimate=pl.CostEstimate(
            flops=2 * total * width * inner * 8 + 10 * total * total * heads * 128,
            bytes_accessed=2 * (3 * total * width + 8 * width * inner + 5 * total * inner),
            transcendentals=heads * total * total,
        ),
        name="attn_backward",
    )(grad_attn, hidden, w_qkv, w_out, qkv, mix, lse)


def ff_kernel(
    block, h_ref, gf_ref, wu_ref, bu_ref, wd_ref,
    part_ref, gh_ref, gwu_ref, gwd_ref, gbu_ref, act_ref, gp_ref,
):
    total, width = h_ref.shape
    inner = wd_ref.shape[0]

    def rows(step, sums):
        at = rows_of(step, block)
        pre = dot(h_ref[at, :], wu_ref[...]) + bu_ref[...]
        square = pre * pre
        tanh_val = jnp.tanh(GELU_C * pre * (1.0 + 0.044715 * square))
        half = 0.5 * (1.0 + tanh_val)
        act = (pre * half).astype(BF)
        slope = half + 0.5 * GELU_C * pre * (1.0 - tanh_val * tanh_val) * (
            1.0 + 3.0 * 0.044715 * square
        )
        grad_pre = dot_nt(gf_ref[at, :], wd_ref[...]) * slope
        grad_low = grad_pre.astype(BF)
        act_ref[at, :] = act
        gp_ref[at, :] = grad_low
        gh_ref[at, :] = dot_nt(grad_low, wu_ref[...]).astype(BF)
        part_ref[at, :] = dot(act, wd_ref[...]).astype(BF)
        return sums + jnp.sum(grad_pre, axis=0, keepdims=True)

    gbu_ref[...] = lax.fori_loop(0, total // block, rows, jnp.zeros((1, inner), F32))

    def down(step, carry):
        at = rows_of(step, 384)
        gwd_ref[at, :] = dot_tn(act_ref[:, at], gf_ref[...]).astype(BF)
        return carry

    lax.fori_loop(0, inner // 384, down, 0)

    def up(step, carry):
        at = rows_of(step, 384)
        gwu_ref[at, :] = dot_tn(h_ref[:, at], gp_ref[...]).astype(BF)
        return carry

    lax.fori_loop(0, width // 384, up, 0)


def feed_forward(hidden, grad_ff, w_up, bias, w_down):
    total, width = hidden.shape
    inner = w_down.shape[0]
    vmem = pl.BlockSpec(memory_space=pltpu.VMEM)
    return pl.pallas_call(
        functools.partial(ff_kernel, 256),
        out_shape=(
            jax.ShapeDtypeStruct((total, width), BF),
            jax.ShapeDtypeStruct((total, width), BF),
            jax.ShapeDtypeStruct((width, inner), BF),
            jax.ShapeDtypeStruct((inner, width), BF),
            jax.ShapeDtypeStruct((1, inner), F32),
        ),
        in_specs=[vmem] * 5,
        out_specs=(vmem,) * 5,
        scratch_shapes=[pltpu.VMEM((total, inner), BF), pltpu.VMEM((total, inner), BF)],
        compiler_params=pltpu.CompilerParams(vmem_limit_bytes=VMEM_LIMIT),
        cost_estimate=pl.CostEstimate(
            flops=12 * total * width * inner,
            bytes_accessed=2 * (4 * total * width + 4 * width * inner),
            transcendentals=total * inner,
        ),
        name="feed_forward",
    )(hidden, grad_ff, w_up, bias, w_down)


def bits_of(count):
    found, bit = [], 1
    while bit < count:
        found.insert(0, bit)
        bit *= 2
    return found


def swap(values, count, bit):
    return lax.ppermute(values, "seq", [(i, i ^ bit) for i in range(count)])


def gather_seq(values, count):
    for bit in bits_of(count):
        values = jnp.concatenate([values, swap(values, count, bit)], axis=0)
    return values


def scatter_seq(values, count):
    for bit in reversed(bits_of(count)):
        half = values.shape[0] // 2
        got = swap(values[half:], count, bit)
        values = values[:half].astype(F32) + got.astype(F32)
        if bit != bits_of(count)[0]:
            values = values.astype(BF)
    return values


def local(n_f, n_s, tokens, condition, w_ada, b_ada, w_qkv, b_qv, w_out, b_out, w_up, b_up,
          w_down, b_down, grad_output):
    lat_dev, seq_loc, width = tokens.shape
    assert lat_dev == 1
    shard = w_qkv.shape[0]
    attn_width = w_qkv.shape[1] // 3
    ff_width = w_up.shape[1]
    inner = attn_width // n_s
    ff_q = ff_width // n_f // n_s
    mods_width = w_ada.shape[1]
    f_at = lax.axis_index("fsdp")
    s_at = lax.axis_index("seq")

    qkv_mine = lax.dynamic_index_in_dim(
        w_qkv.reshape(shard, 3, n_s, inner), s_at, 2, keepdims=False
    ).reshape(shard, 3 * inner)
    full_qkv = lax.all_gather(qkv_mine, "fsdp", axis=0, tiled=True)

    packed = jnp.concatenate(
        [condition.reshape(-1)]
        + [part.astype(F32).reshape(-1) for part in (b_qv, b_out, b_up, b_down)]
    )
    packed_all = lax.all_gather(packed, "fsdp", axis=0)
    sizes = [width, 2 * (attn_width // n_f), width // n_f, ff_width // n_f, width // n_f]
    parts, start = [], 0
    for size in sizes:
        parts.append(packed_all[:, start : start + size])
        start += size
    cond_all, bqv_all, bout_all, bup_all, bdown_all = parts
    full_bqv = bqv_all.reshape(n_f, 2, attn_width // n_f).transpose(1, 0, 2).reshape(2, n_s, inner)
    bqv_mine = lax.dynamic_index_in_dim(full_bqv, s_at, 1, keepdims=False)
    bias_qkv = jnp.concatenate([bqv_mine[0], jnp.zeros((inner,), F32), bqv_mine[1]])[None]
    full_bout = bout_all.reshape(1, width)
    full_bdown = bdown_all.reshape(1, width)
    bias_up = lax.dynamic_index_in_dim(
        bup_all.reshape(n_f, n_s, ff_q), s_at, 1, keepdims=False
    ).reshape(1, n_f * ff_q)

    act_all = (cond_all * jax.nn.sigmoid(cond_all)).astype(BF)
    act_rows = lax.dynamic_index_in_dim(
        act_all.reshape(n_f, n_f, shard), f_at, 1, keepdims=False
    )
    mods_part = dot(act_rows, w_ada)
    own_bias = lax.dynamic_update_slice(
        jnp.zeros((1, mods_width), F32), b_ada.astype(F32)[None], (0, f_at * b_ada.shape[0])
    )
    mods = lax.psum_scatter(mods_part + own_bias, "fsdp", scatter_dimension=0, tiled=True)
    shift_attn, scale_attn, gate_attn, shift_ff, scale_ff, gate_ff = [
        mods[:, i * width : (i + 1) * width] for i in range(6)
    ]

    out_rows = w_out.shape[0] // n_s
    out_mine = lax.dynamic_index_in_dim(
        w_out.reshape(n_s, out_rows, width), s_at, 0, keepdims=False
    )
    out_quarter = lax.all_gather(out_mine, "fsdp", axis=0)
    up_mine = lax.dynamic_index_in_dim(
        w_up.reshape(shard, n_f, n_s, ff_q), s_at, 2, keepdims=False
    ).reshape(shard, n_f * ff_q)
    full_up = lax.all_gather(up_mine, "fsdp", axis=0, tiled=True)
    down_mine = lax.dynamic_index_in_dim(
        w_down.reshape(n_s, ff_q, width), s_at, 0, keepdims=False
    )
    full_down = lax.all_gather(down_mine, "fsdp", axis=0, tiled=True)
    out_heads = lax.all_to_all(
        out_quarter.reshape(n_s, n_f // n_s, out_rows, width), "seq", 0, 0, tiled=True
    )
    full_out = out_heads.transpose(1, 0, 2, 3).reshape(inner, width)

    source = tokens.reshape(seq_loc, width).astype(F32)
    grad_y = grad_output.reshape(seq_loc, width).astype(F32)
    normed1, inv1 = layer_norm(source)
    hidden1 = (normed1 * (1.0 + scale_attn) + shift_attn).astype(BF)
    hidden1_all = gather_seq(hidden1, n_s)
    grad_ff = grad_y * gate_ff
    grad_ff_all = gather_seq(grad_ff.astype(BF), n_s)
    part, qkv, mix, lse = attn_forward(hidden1_all, full_qkv, bias_qkv, full_out)
    attn_out = scatter_seq(part, n_s) + full_bout
    resid1 = source + gate_attn * attn_out
    normed2, inv2 = layer_norm(resid1)
    hidden2 = (normed2 * (1.0 + scale_ff) + shift_ff).astype(BF)
    hidden2_all = gather_seq(hidden2, n_s)
    ff_part, gh2_part, gw_up, gw_down, gb_up = feed_forward(
        hidden2_all, grad_ff_all, full_up, bias_up, full_down
    )
    grad_h2 = scatter_seq(gh2_part, n_s)
    s_down = lax.psum_scatter(gw_down, "fsdp", scatter_dimension=0, tiled=True)
    s_up = lax.psum_scatter(gw_up, "fsdp", scatter_dimension=0, tiled=True)

    grad_resid1 = grad_y + norm_back(grad_h2 * (1.0 + scale_ff), normed2, inv2)
    grad_attn = grad_resid1 * gate_attn
    grad_attn_all = gather_seq(grad_attn.astype(BF), n_s)
    ff_out = scatter_seq(ff_part, n_s) + full_bdown
    output = (resid1 + gate_ff * ff_out).astype(BF)
    gh1_part, gw_qkv, gw_out, gb_qkv = attn_backward(
        grad_attn_all, hidden1_all, full_qkv, full_out, qkv, mix, lse
    )
    grad_h1 = scatter_seq(gh1_part, n_s)
    s_qkv = lax.psum_scatter(gw_qkv, "fsdp", scatter_dimension=0, tiled=True)
    gw_out_q = lax.all_to_all(
        gw_out.reshape(n_f // n_s, n_s, out_rows, width).transpose(1, 0, 2, 3),
        "seq", 0, 0, tiled=True,
    )
    s_out = lax.psum_scatter(
        gw_out_q.reshape(n_f * out_rows, width), "fsdp", scatter_dimension=0, tiled=True
    )
    grad_tokens = (grad_resid1 + norm_back(grad_h1 * (1.0 + scale_attn), normed1, inv1)).astype(BF)

    token_sums = [
        grad_h1, grad_h1 * normed1, grad_resid1 * attn_out, grad_h2, grad_h2 * normed2,
        grad_y * ff_out,
    ]
    grad_mods = jnp.concatenate([jnp.sum(value, axis=0) for value in token_sums])
    grad_mods = grad_mods.astype(BF).astype(F32)
    gb_qv = jnp.stack([gb_qkv[0, :inner], gb_qkv[0, 2 * inner :]]).reshape(2, 1, inner)
    gb_qv = lax.dynamic_update_slice(jnp.zeros((2, n_s, inner), F32), gb_qv, (0, s_at, 0))
    gb_up_full = lax.dynamic_update_slice(
        jnp.zeros((n_f, n_s, ff_q), F32), gb_up.reshape(n_f, 1, ff_q), (0, s_at, 0)
    )
    small = jnp.concatenate(
        [grad_mods, jnp.sum(grad_ff, axis=0), jnp.sum(grad_attn, axis=0), gb_up_full.reshape(-1),
         gb_qv.reshape(-1)]
    )
    small_all = lax.all_gather(lax.psum(small, "seq"), "fsdp", axis=0)
    mods_all = small_all[:, :mods_width]
    total = jnp.sum(small_all, axis=0)
    parts, start = [], 0
    for size in (mods_width, width, width, ff_width):
        piece = size // n_f
        parts.append(lax.dynamic_slice(total, (start + f_at * piece,), (piece,)))
        start += size
    t_bada, t_bdown, t_bout, t_bup = parts
    t_bqv = lax.dynamic_slice(
        total[start:].reshape(2, attn_width), (0, f_at * (attn_width // n_f)), (2, attn_width // n_f)
    )
    mods_low = mods_all.astype(BF)
    t_wada = dot_tn(act_rows, mods_low)
    cond_rows = dot_nt(mods_low, w_ada)
    grad_act = lax.all_gather(cond_rows, "fsdp", axis=1, tiled=True)
    grad_act = lax.dynamic_slice_in_dim(grad_act, f_at, 1, 0)
    cond_sig = jax.nn.sigmoid(condition)
    t_cond = grad_act * cond_sig * (1.0 + condition * (1.0 - cond_sig))

    a_down = lax.all_gather(s_down, "seq", axis=0, tiled=True)
    a_up = lax.all_gather(s_up, "seq", axis=0)
    a_qkv = lax.all_gather(s_qkv, "seq", axis=0)
    a_out = lax.all_gather(s_out, "seq", axis=0, tiled=True)
    t_wup = a_up.reshape(n_s, shard, n_f, ff_q).transpose(1, 2, 0, 3).reshape(shard, ff_width)
    t_wqkv = a_qkv.reshape(n_s, shard, 3, inner).transpose(1, 2, 0, 3).reshape(shard, -1)
    return (
        output[None],
        grad_tokens[None],
        t_cond,
        t_wada,
        t_bada,
        t_wqkv.astype(F32),
        t_bqv,
        a_out.astype(F32),
        t_bout,
        t_wup.astype(F32),
        t_bup,
        a_down.astype(F32),
        t_bdown,
    )


def solution(mesh):
    in_specs = (
        P("fsdp", "seq", None),
        P("fsdp", None),
        P("fsdp", None),
        P("fsdp"),
        P("fsdp", None),
        P(None, "fsdp"),
        P("fsdp", None),
        P("fsdp"),
        P("fsdp", None),
        P("fsdp"),
        P("fsdp", None),
        P("fsdp"),
        P("fsdp", "seq", None),
    )
    out_specs = (
        P("fsdp", "seq", None),
        P("fsdp", "seq", None),
        P("fsdp", None),
        P("fsdp", None),
        P("fsdp"),
        P("fsdp", None),
        P(None, "fsdp"),
        P("fsdp", None),
        P("fsdp"),
        P("fsdp", None),
        P("fsdp"),
        P("fsdp", None),
        P("fsdp"),
    )
    body = functools.partial(local, mesh.shape["fsdp"], mesh.shape["seq"])
    return jax.shard_map(body, mesh=mesh, in_specs=in_specs, out_specs=out_specs, check_vma=False)
```
